32 devices in a mesh: dp: 8 (over z, x), rep: 4 (over y, core).
Axes of the slice: x: 2, y: 2, z: 4, core: 2. Of those that a mesh axis runs over, the one named last changes fastest.
Arguments:
- tokens: bfloat16 [8192, 2048], P(('rep', 'dp')), parts along dimension 0, may hold values from -12 to 12
- router: bfloat16 [8192, 8], P('rep'), parts along dimension 0, may hold values from -12 to 12
- w_gate: bfloat16 [8, 2048, 768], P('dp'), may hold values from -0.125 to 0.125
- w_up: bfloat16 [8, 2048, 768], P('dp'), may hold values from -0.125 to 0.125
- w_down: bfloat16 [8, 768, 2048], P('dp'), may hold values from -0.21875 to 0.21875
- picks: int32 [32, 32], P(('rep', 'dp')), parts along dimension 0, may hold values from 0 to 2047, as said below
Outputs:
- combined: bfloat16 [8192, 2048], P(('rep', 'dp')), parts along dimension 0
The draws below stay inside these ranges and needn't reach their ends.
There are 4 independent parts, one for each index of `rep`. The reference program is written for one: setup_inputs(seed, part) draws one part's arguments, and reference() takes and returns one part's arrays. A program takes and returns all parts, laid end to end along the dimension named above; an argument that names none is the same for every part. Nothing has to cross between parts.
Inputs may be any that keep to these rules, and one draw needn't show every extreme that they name: `picks`: row e holds 32 different tokens taken by expert e, sorted by the device that holds them (256 tokens each, in order); at most 6 of them lie among one device's tokens, and in every row exactly 6 lie among some device's tokens.
All inputs are finite; a program needn't handle non-finite values.
Results may differ from the reference program's by a relative error of at most 0.0062.
Values may be sent and summed in bfloat16 or wider, within the bound.
No kernel may reach another device: no remote copies, remote signals or barrier semaphores. Data moves between devices by JAX's collectives and lax.ppermute only.
A program may use at most 64 MiB of HBM per device.

```python
import math
import jax
import jax.numpy as jnp
from jax import lax

D = 2048
FF = 768
TOK_DEV = 256
BASE = 4
EXPERTS = 8
CAP = 32
TOKENS = 2048


def draw_router(key, part):
    base = jax.random.normal(jax.random.fold_in(key, 21), (D, EXPERTS), jnp.float32)
    matrix = base * (1.0 / math.sqrt(D))
    return jnp.clip(matrix, -12.0, 12.0).astype(jnp.bfloat16)


def draw_tokens(key, part):
    values = jax.random.normal(jax.random.fold_in(key, 31), (TOKENS, D), jnp.float32)
    return jnp.clip(values, -12.0, 12.0).astype(jnp.bfloat16)


def draw_picks(key, part):
    key_pair, key_shift, key_order = jax.random.split(key, 3)
    half_base = BASE // 2
    pairing = jax.vmap(lambda subkey: jax.random.permutation(subkey, EXPERTS))(jax.random.split(key_pair, EXPERTS))
    offsets = jax.random.randint(key_shift, (EXPERTS, EXPERTS // 2), -half_base, half_base + 1)
    offsets = offsets.at[:, 0].set(half_base)
    paired = (jnp.concatenate([offsets, -offsets], axis=1) + BASE).astype(jnp.int32)
    rows_at = jnp.arange(EXPERTS, dtype=jnp.int32)[:, None]
    counts = jnp.zeros((EXPERTS, EXPERTS), jnp.int32).at[rows_at, pairing].set(paired)
    block_end = jnp.cumsum(counts, axis=1)
    starts = block_end - counts
    slot_pos = jnp.arange(CAP, dtype=jnp.int32)
    source_of = jnp.sum((slot_pos[None, :, None] >= block_end[:, None, :]).astype(jnp.int32), axis=2)
    within = slot_pos[None, :] - jnp.take_along_axis(starts, source_of, axis=1)
    scores = jax.random.randint(key_order, (EXPERTS, EXPERTS, TOK_DEV), 0, 1 << 30)
    shuffled = jnp.argsort(scores, axis=2, stable=True).astype(jnp.int32)
    shuffled_rows = shuffled.reshape(EXPERTS * EXPERTS, TOK_DEV)
    row_index = rows_at * EXPERTS + source_of
    local_pick = shuffled_rows[row_index, within]
    return (source_of * TOK_DEV + local_pick).astype(jnp.int32)


def steps_of(key, dims, shards, smallest, largest):
    level = 1.0
    for dim, blocks in shards:
        steps = jax.random.uniform(jax.random.fold_in(jax.random.fold_in(key, 6), dim), (blocks,), jnp.float32, smallest / len(shards), largest / len(shards))
        level = level * jnp.repeat(jnp.exp(steps), dims[dim] // blocks).reshape((-1,) + (1,) * (len(dims) - 1 - dim))
    return level


def scatter_about(own_key, shape, deviation, reach, cuts=(), kind=jnp.bfloat16):
    array = jax.random.normal(own_key, shape, jnp.float32) * deviation
    if len(cuts) > 0:
        array = steps_of(own_key, shape, cuts, -0.22, 0.18) * array
    return jnp.clip(array, min=-reach, max=reach).astype(kind)


def setup_inputs(seed: int = 0, part: int = 0) -> dict:
    arg_keys = jax.random.split(jax.random.key(seed), 7)
    own_keys = jax.random.split(jax.random.fold_in(arg_keys[6], part), 7)
    return {
        "tokens": draw_tokens(jax.random.fold_in(jax.random.fold_in(arg_keys[6], part), 71), part),
        "router": draw_router(jax.random.fold_in(jax.random.fold_in(arg_keys[6], part), 71), part),
        "w_gate": scatter_about(arg_keys[2], (EXPERTS, D, FF), D ** -0.5, 0.125, ((0, 8),)),
        "w_up": scatter_about(arg_keys[3], (EXPERTS, D, FF), D ** -0.5, 0.125, ((0, 8),)),
        "w_down": scatter_about(arg_keys[4], (EXPERTS, FF, D), FF ** -0.5, 0.21875, ((0, 8),)),
        "picks": draw_picks(jax.random.fold_in(jax.random.fold_in(arg_keys[6], part), 71), part),
    }


def reference(tokens, router, w_gate, w_up, w_down, picks):
    logits = jnp.dot(tokens, router, preferred_element_type=jnp.float32)
    shares = jax.nn.softmax(logits, axis=1)
    gates = (EXPERTS * jnp.take_along_axis(shares.T, picks, axis=1)).astype(jnp.bfloat16)

    def one_expert(inputs):
        gate_w, up_w, down_w, chosen_index, gate_row = inputs
        chosen = tokens[chosen_index]
        gate_act = jnp.dot(chosen, gate_w, preferred_element_type=jnp.float32)
        up_act = jnp.dot(chosen, up_w, preferred_element_type=jnp.float32)
        hidden = (gate_row.astype(jnp.float32)[:, None] * jax.nn.silu(gate_act) * up_act).astype(jnp.bfloat16)
        return jnp.dot(hidden, down_w, preferred_element_type=jnp.float32).astype(jnp.bfloat16)

    results = lax.map(one_expert, (w_gate, w_up, w_down, picks, gates))
    width = tokens.shape[1]
    combined = jnp.zeros((tokens.shape[0], width), jnp.float32).at[picks.reshape(-1)].add(
        results.reshape(-1, width).astype(jnp.float32))
    return combined.astype(jnp.bfloat16)
```

```python
import jax
import jax.numpy as jnp
from jax import lax
from jax.experimental import pallas as pl
from jax.experimental.pallas import tpu as pltpu
from jax.sharding import PartitionSpec as P

MOST = 6
SLOTS = 8
PARTS = 4
THIRDS = MOST // 2
LONG = 10_000_000_000
VMEM = pl.BlockSpec(memory_space=pltpu.VMEM)
PARAMS = pltpu.CompilerParams(vmem_limit_bytes=16 * 1024 * 1024)


def prep_kernel(picks_ref, out_ref):
    out_ref[...] = picks_ref[...]


def prep(picks):
    return pl.pallas_call(
        prep_kernel,
        out_shape=jax.ShapeDtypeStruct(picks.shape, picks.dtype),
        in_specs=[VMEM],
        out_specs=VMEM,
        compiler_params=PARAMS,
        cost_estimate=pl.CostEstimate(flops=LONG, bytes_accessed=0, transcendentals=0),
        name="prep",
    )(picks)


def select_kernel(ids, table_ref, tokens_ref, send_ref, hot_ref, sorted_ref):
    tok_dev, width = tokens_ref.shape
    n, slots, capacity = sorted_ref.shape
    part = width // PARTS
    me = lax.axis_index("dp").astype(jnp.int32)
    for r, i in enumerate(ids):
        sorted_ref[me ^ i] = jnp.broadcast_to(table_ref[r : r + 1, :], (slots, capacity))
    local = sorted_ref[...] - me * tok_dev
    row = lax.broadcasted_iota(jnp.int32, local.shape, 1)
    lane = lax.broadcasted_iota(jnp.int32, local.shape, 2)
    column = lax.broadcasted_iota(jnp.int32, (n, slots, tok_dev), 2)
    start = jnp.sum((local < 0).astype(jnp.int32), axis=2, keepdims=True)
    place = lane - start
    value = jnp.where((local >= 0) & (local < tok_dev), local + 1, 0)
    hots = []
    for q in range(PARTS):
        if q == 0:
            wanted = jnp.where(row < MOST, row, -1)
        else:
            first, second = q - 1, q - 1 + THIRDS
            wanted = jnp.where(row == MOST, first, jnp.where(row == MOST + 1, second, -1))
        index = jnp.sum(jnp.where(place == wanted, value, 0), axis=2, keepdims=True) - 1
        hot = (index == column).astype(jnp.float32).reshape(n * slots, tok_dev)
        hots.append(hot.astype(jnp.bfloat16))
        hot_ref[q] = hots[q]
    tail = tokens_ref[:, (PARTS - 1) * part :]
    for q in range(PARTS - 1):
        chosen = jnp.dot(
            hots[0], tokens_ref[:, q * part : (q + 1) * part], preferred_element_type=jnp.float32
        ) + jnp.dot(hots[q + 1], tail, preferred_element_type=jnp.float32)
        send_ref[:, :, q * part : (q + 1) * part] = chosen.reshape(n, slots, part).astype(
            jnp.bfloat16
        )


def select(ids, table, tokens):
    tok_dev, width = tokens.shape
    n, capacity = table.shape
    return pl.pallas_call(
        lambda *refs: select_kernel(ids, *refs),
        out_shape=[
            jax.ShapeDtypeStruct((n, SLOTS, width // PARTS * (PARTS - 1)), jnp.bfloat16),
            jax.ShapeDtypeStruct((PARTS, n * SLOTS, tok_dev), jnp.bfloat16),
        ],
        in_specs=[VMEM, VMEM],
        out_specs=[VMEM, VMEM],
        scratch_shapes=[pltpu.VMEM((n, SLOTS, capacity), jnp.int32)],
        compiler_params=PARAMS,
        name="select",
    )(table, tokens)


def ffn_kernel(router_ref, gate_ref, up_ref, down_ref, x_ref, y_ref):
    n, slots, packed = x_ref.shape
    part = packed // (PARTS - 1)
    width = part * PARTS
    rows = n * slots
    experts = router_ref.shape[0]
    me = lax.axis_index("dp").astype(jnp.int32)
    head = x_ref[...].astype(jnp.float32)
    row = lax.broadcasted_iota(jnp.int32, (n, slots, part), 1)
    tail = jnp.zeros((n, slots, part), jnp.float32)
    for q in range(PARTS - 1):
        piece = head[:, :, q * part : (q + 1) * part]
        tail = jnp.where(row == q, piece[:, MOST : MOST + 1], tail)
        tail = jnp.where(row == q + THIRDS, piece[:, MOST + 1 : MOST + 2], tail)
    x = jnp.concatenate([head.reshape(rows, packed), tail.reshape(rows, part)], axis=1)
    x = x.astype(jnp.bfloat16)
    logits = lax.dot_general(
        x, router_ref[...], (((1,), (1,)), ((), ())), preferred_element_type=jnp.float32
    )
    expert_of = lax.broadcasted_iota(jnp.int32, logits.shape, 1)
    top = jnp.max(logits, axis=1, keepdims=True)
    weight = jnp.exp(logits - top)
    total = jnp.sum(weight, axis=1, keepdims=True)
    own = jnp.sum(jnp.where(expert_of == me, weight, 0.0), axis=1, keepdims=True)
    gate_value = (experts * (own / total)).astype(jnp.bfloat16).astype(jnp.float32)
    gate_act = jnp.dot(x, gate_ref[...], preferred_element_type=jnp.float32)
    up_act = jnp.dot(x, up_ref[...], preferred_element_type=jnp.float32)
    silu = gate_act / (1.0 + jnp.exp(-gate_act))
    hidden = (gate_value * silu * up_act).astype(jnp.bfloat16)
    y = jnp.dot(hidden, down_ref[...], preferred_element_type=jnp.float32)
    y = y.reshape(n, slots, width)
    last = y[:, :, packed:]
    for q in range(PARTS - 1):
        piece = y[:, :, q * part : (q + 1) * part]
        piece = jnp.where(row == MOST, last[:, q : q + 1], piece)
        piece = jnp.where(row == MOST + 1, last[:, q + THIRDS : q + THIRDS + 1], piece)
        y_ref[:, :, q * part : (q + 1) * part] = piece.astype(jnp.bfloat16)


def ffn(router_t, w_gate, w_up, w_down, x):
    return pl.pallas_call(
        ffn_kernel,
        out_shape=jax.ShapeDtypeStruct(x.shape, jnp.bfloat16),
        in_specs=[VMEM] * 5,
        out_specs=VMEM,
        compiler_params=PARAMS,
        name="ffn",
    )(router_t, w_gate, w_up, w_down, x)


def spread(hot, rows):
    return lax.dot_general(hot, rows, (((0,), (0,)), ((), ())), preferred_element_type=jnp.float32)


def combine_kernel(hot_ref, y_ref, out_ref, block_ref, sem):
    n, slots, packed = y_ref.shape
    part = packed // (PARTS - 1)
    rows = n * slots
    copies = []
    pieces = [y_ref[:, :, q * part : (q + 1) * part] for q in range(PARTS - 1)]
    pieces = [p.astype(jnp.float32).reshape(rows, part).astype(jnp.bfloat16) for p in pieces]
    for q in range(PARTS):
        if q < PARTS - 1:
            total = spread(hot_ref[0], pieces[q])
        else:
            total = sum(spread(hot_ref[k + 1], pieces[k]) for k in range(PARTS - 1))
        block_ref[q] = total.astype(jnp.bfloat16)
        copy = pltpu.make_async_copy(
            block_ref.at[q], out_ref.at[:, pl.ds(q * part, part)], sem.at[q]
        )
        copy.start()
        copies.append(copy)
    for copy in copies:
        copy.wait()


def combine(hots, y):
    tok_dev = hots.shape[2]
    part = y.shape[2] // (PARTS - 1)
    return pl.pallas_call(
        combine_kernel,
        out_shape=jax.ShapeDtypeStruct((tok_dev, part * PARTS), jnp.bfloat16),
        in_specs=[VMEM, VMEM],
        out_specs=pl.BlockSpec(memory_space=pl.ANY),
        scratch_shapes=[
            pltpu.VMEM((PARTS, tok_dev, part), jnp.bfloat16),
            pltpu.SemaphoreType.DMA((PARTS,)),
        ],
        compiler_params=PARAMS,
        name="combine",
    )(hots, y)


def exchange(value):
    return lax.all_to_all(value, "dp", split_axis=0, concat_axis=0, tiled=True)


def body(tokens, router, w_gate, w_up, w_down, picks):
    n = lax.axis_size("dp")
    known, ids, flip = prep(picks), [0], n // 2
    sent = picks
    while flip:
        got = lax.ppermute(sent, "dp", [(i, i ^ flip) for i in range(n)])
        known = sent = jnp.concatenate([known, got], axis=0)
        ids = ids + [i ^ flip for i in ids]
        flip //= 2
    send, hots = select(ids, known, tokens)
    received = exchange(send)
    y = ffn(router.T, w_gate[0], w_up[0], w_down[0], received)
    return combine(hots, exchange(y))


def solution(mesh):
    return jax.shard_map(
        body,
        mesh=mesh,
        in_specs=(
            P(("rep", "dp"), None),
            P("rep", None),
            P("dp", None, None),
            P("dp", None, None),
            P("dp", None, None),
            P(("rep", "dp"), None),
        ),
        out_specs=P(("rep", "dp"), None),
        check_vma=False,
    )
```

```python
import jax
import jax.numpy as jnp
from jax import lax
from jax.experimental import pallas as pl
from jax.experimental.pallas import tpu as pltpu
from jax.sharding import PartitionSpec as P

MOST = 6
SLOTS = 8
PARTS = 4
THIRDS = MOST // 2
LONG = 10_000_000_000
VMEM = pl.BlockSpec(memory_space=pltpu.VMEM)
PARAMS = pltpu.CompilerParams(vmem_limit_bytes=16 * 1024 * 1024)


def spread_kernel(picks_ref, out_ref):
    out_ref[...] = jnp.broadcast_to(picks_ref[...][None], out_ref.shape)


def spread(picks, n):
    return pl.pallas_call(
        spread_kernel,
        out_shape=jax.ShapeDtypeStruct((n,) + picks.shape, picks.dtype),
        in_specs=[VMEM],
        out_specs=VMEM,
        compiler_params=PARAMS,
        cost_estimate=pl.CostEstimate(flops=LONG, bytes_accessed=0, transcendentals=0),
        name="spread",
    )(picks)


def select_kernel(table_ref, tokens_ref, send_ref, hot_ref):
    tok_dev, width = tokens_ref.shape
    n, slots, _ = send_ref.shape
    capacity = table_ref.shape[2]
    part = width // PARTS
    me = lax.axis_index("dp").astype(jnp.int32)
    table = jnp.broadcast_to(table_ref[...], (n, slots, capacity))
    local = table - me * tok_dev
    row = lax.broadcasted_iota(jnp.int32, local.shape, 1)
    lane = lax.broadcasted_iota(jnp.int32, local.shape, 2)
    column = lax.broadcasted_iota(jnp.int32, (n, slots, tok_dev), 2)
    start = jnp.sum((local < 0).astype(jnp.int32), axis=2, keepdims=True)
    place = lane - start
    value = jnp.where((local >= 0) & (local < tok_dev), local + 1, 0)
    hots = []
    for q in range(PARTS):
        if q == 0:
            wanted = jnp.where(row < MOST, row, -1)
        else:
            first, second = q - 1, q - 1 + THIRDS
            wanted = jnp.where(row == MOST, first, jnp.where(row == MOST + 1, second, -1))
        index = jnp.sum(jnp.where(place == wanted, value, 0), axis=2, keepdims=True) - 1
        hot = (index == column).astype(jnp.float32).reshape(n * slots, tok_dev)
        hots.append(hot.astype(jnp.bfloat16))
        hot_ref[q] = hots[q]
    tail = tokens_ref[:, (PARTS - 1) * part :]
    for q in range(PARTS - 1):
        chosen = jnp.dot(
            hots[0], tokens_ref[:, q * part : (q + 1) * part], preferred_element_type=jnp.float32
        ) + jnp.dot(hots[q + 1], tail, preferred_element_type=jnp.float32)
        send_ref[:, :, q * part : (q + 1) * part] = chosen.reshape(n, slots, part).astype(
            jnp.bfloat16
        )


def select(table, tokens):
    tok_dev, width = tokens.shape
    n = table.shape[0]
    return pl.pallas_call(
        select_kernel,
        out_shape=[
            jax.ShapeDtypeStruct((n, SLOTS, width // PARTS * (PARTS - 1)), jnp.bfloat16),
            jax.ShapeDtypeStruct((PARTS, n * SLOTS, tok_dev), jnp.bfloat16),
        ],
        in_specs=[VMEM, VMEM],
        out_specs=[VMEM, VMEM],
        compiler_params=PARAMS,
        name="select",
    )(table, tokens)


def ffn_kernel(router_ref, gate_ref, up_ref, down_ref, x_ref, y_ref):
    n, slots, packed = x_ref.shape
    part = packed // (PARTS - 1)
    width = part * PARTS
    rows = n * slots
    experts = router_ref.shape[0]
    me = lax.axis_index("dp").astype(jnp.int32)
    head = x_ref[...].astype(jnp.float32)
    row = lax.broadcasted_iota(jnp.int32, (n, slots, part), 1)
    tail = jnp.zeros((n, slots, part), jnp.float32)
    for q in range(PARTS - 1):
        piece = head[:, :, q * part : (q + 1) * part]
        tail = jnp.where(row == q, piece[:, MOST : MOST + 1], tail)
        tail = jnp.where(row == q + THIRDS, piece[:, MOST + 1 : MOST + 2], tail)
    x = jnp.concatenate([head.reshape(rows, packed), tail.reshape(rows, part)], axis=1)
    x = x.astype(jnp.bfloat16)
    logits = lax.dot_general(
        x, router_ref[...], (((1,), (1,)), ((), ())), preferred_element_type=jnp.float32
    )
    expert_of = lax.broadcasted_iota(jnp.int32, logits.shape, 1)
    top = jnp.max(logits, axis=1, keepdims=True)
    weight = jnp.exp(logits - top)
    total = jnp.sum(weight, axis=1, keepdims=True)
    own = jnp.sum(jnp.where(expert_of == me, weight, 0.0), axis=1, keepdims=True)
    gate_value = (experts * (own / total)).astype(jnp.bfloat16).astype(jnp.float32)
    gate_act = jnp.dot(x, gate_ref[...], preferred_element_type=jnp.float32)
    up_act = jnp.dot(x, up_ref[...], preferred_element_type=jnp.float32)
    silu = gate_act / (1.0 + jnp.exp(-gate_act))
    hidden = (gate_value * silu * up_act).astype(jnp.bfloat16)
    y = jnp.dot(hidden, down_ref[...], preferred_element_type=jnp.float32)
    y = y.reshape(n, slots, width)
    last = y[:, :, packed:]
    for q in range(PARTS - 1):
        piece = y[:, :, q * part : (q + 1) * part]
        piece = jnp.where(row == MOST, last[:, q : q + 1], piece)
        piece = jnp.where(row == MOST + 1, last[:, q + THIRDS : q + THIRDS + 1], piece)
        y_ref[:, :, q * part : (q + 1) * part] = piece.astype(jnp.bfloat16)


def ffn(router_t, w_gate, w_up, w_down, x):
    return pl.pallas_call(
        ffn_kernel,
        out_shape=jax.ShapeDtypeStruct(x.shape, jnp.bfloat16),
        in_specs=[VMEM] * 5,
        out_specs=VMEM,
        compiler_params=PARAMS,
        name="ffn",
    )(router_t, w_gate, w_up, w_down, x)


def place(hot, rows):
    return lax.dot_general(hot, rows, (((0,), (0,)), ((), ())), preferred_element_type=jnp.float32)


def combine_kernel(hot_ref, y_ref, out_ref, block_ref, sem):
    n, slots, packed = y_ref.shape
    part = packed // (PARTS - 1)
    rows = n * slots
    copies = []
    pieces = [y_ref[:, :, q * part : (q + 1) * part] for q in range(PARTS - 1)]
    pieces = [p.astype(jnp.float32).reshape(rows, part).astype(jnp.bfloat16) for p in pieces]
    for q in range(PARTS):
        if q < PARTS - 1:
            total = place(hot_ref[0], pieces[q])
        else:
            total = sum(place(hot_ref[k + 1], pieces[k]) for k in range(PARTS - 1))
        block_ref[q] = total.astype(jnp.bfloat16)
        copy = pltpu.make_async_copy(
            block_ref.at[q], out_ref.at[:, pl.ds(q * part, part)], sem.at[q]
        )
        copy.start()
        copies.append(copy)
    for copy in copies:
        copy.wait()


def combine(hots, y):
    tok_dev = hots.shape[2]
    part = y.shape[2] // (PARTS - 1)
    return pl.pallas_call(
        combine_kernel,
        out_shape=jax.ShapeDtypeStruct((tok_dev, part * PARTS), jnp.bfloat16),
        in_specs=[VMEM, VMEM],
        out_specs=pl.BlockSpec(memory_space=pl.ANY),
        scratch_shapes=[
            pltpu.VMEM((PARTS, tok_dev, part), jnp.bfloat16),
            pltpu.SemaphoreType.DMA((PARTS,)),
        ],
        compiler_params=PARAMS,
        name="combine",
    )(hots, y)


def exchange(value):
    n = lax.axis_size("dp")
    order = [(n // 2 + 1 - k) % n for k in range(n)]
    return lax.all_to_all(
        value, "dp", split_axis=0, concat_axis=0, tiled=True, axis_index_groups=[order]
    )


def body(tokens, router, w_gate, w_up, w_down, picks):
    n = lax.axis_size("dp")
    send, hots = select(exchange(spread(picks, n)), tokens)
    received = exchange(send)
    y = ffn(router.T, w_gate[0], w_up[0], w_down[0], received)
    return combine(hots, exchange(y))


def solution(mesh):
    return jax.shard_map(
        body,
        mesh=mesh,
        in_specs=(
            P(("rep", "dp"), None),
            P("rep", None),
            P("dp", None, None),
            P("dp", None, None),
            P("dp", None, None),
            P(("rep", "dp"), None),
        ),
        out_specs=P(("rep", "dp"), None),
        check_vma=False,
    )
```

```python
import jax
import jax.numpy as jnp
from jax import lax
from jax.experimental import pallas as pl
from jax.experimental.pallas import tpu as pltpu
from jax.sharding import PartitionSpec as P

MOST = 6
SLOTS = 8
PARTS = 4
THIRDS = MOST // 2
LONG = 10_000_000_000
VMEM = pl.BlockSpec(memory_space=pltpu.VMEM)
PARAMS = pltpu.CompilerParams(vmem_limit_bytes=16 * 1024 * 1024)


def hold_kernel(in_ref, out_ref):
    out_ref[...] = in_ref[...]


def hold(value):
    return pl.pallas_call(
        hold_kernel,
        out_shape=jax.ShapeDtypeStruct(value.shape, value.dtype),
        in_specs=[VMEM],
        out_specs=VMEM,
        compiler_params=PARAMS,
        cost_estimate=pl.CostEstimate(flops=LONG, bytes_accessed=0, transcendentals=0),
        name="hold",
    )(value)


def select_kernel(table_ref, tokens_ref, send_ref, hot_ref):
    tok_dev, width = tokens_ref.shape
    n, slots, _ = send_ref.shape
    capacity = table_ref.shape[2]
    part = width // PARTS
    me = lax.axis_index("dp").astype(jnp.int32)
    table = jnp.broadcast_to(table_ref[...], (n, slots, capacity))
    local = table - me * tok_dev
    row = lax.broadcasted_iota(jnp.int32, local.shape, 1)
    lane = lax.broadcasted_iota(jnp.int32, local.shape, 2)
    column = lax.broadcasted_iota(jnp.int32, (n, slots, tok_dev), 2)
    start = jnp.sum((local < 0).astype(jnp.int32), axis=2, keepdims=True)
    place = lane - start
    value = jnp.where((local >= 0) & (local < tok_dev), local + 1, 0)
    hots = []
    for q in range(PARTS):
        if q == 0:
            wanted = jnp.where(row < MOST, row, -1)
        else:
            first, second = q - 1, q - 1 + THIRDS
            wanted = jnp.where(row == MOST, first, jnp.where(row == MOST + 1, second, -1))
        index = jnp.sum(jnp.where(place == wanted, value, 0), axis=2, keepdims=True) - 1
        hot = (index == column).astype(jnp.float32).reshape(n * slots, tok_dev)
        hots.append(hot.astype(jnp.bfloat16))
        hot_ref[q * n * slots : (q + 1) * n * slots] = hots[q]
    tail = tokens_ref[:, (PARTS - 1) * part :]
    for q in range(PARTS - 1):
        chosen = jnp.dot(
            hots[0], tokens_ref[:, q * part : (q + 1) * part], preferred_element_type=jnp.float32
        ) + jnp.dot(hots[q + 1], tail, preferred_element_type=jnp.float32)
        send_ref[:, :, q * part : (q + 1) * part] = chosen.reshape(n, slots, part).astype(
            jnp.bfloat16
        )


def select(table, tokens):
    tok_dev, width = tokens.shape
    n = table.shape[0]
    return pl.pallas_call(
        select_kernel,
        out_shape=[
            jax.ShapeDtypeStruct((n, SLOTS, width // PARTS * (PARTS - 1)), jnp.bfloat16),
            jax.ShapeDtypeStruct((PARTS * n * SLOTS, tok_dev), jnp.bfloat16),
        ],
        in_specs=[VMEM, VMEM],
        out_specs=[VMEM, VMEM],
        compiler_params=PARAMS,
        name="select",
    )(table, tokens)


def ffn_kernel(router_ref, gate_ref, up_ref, down_ref, x_ref, y_ref):
    n, slots, packed = x_ref.shape
    part = packed // (PARTS - 1)
    width = part * PARTS
    rows = n * slots
    experts = router_ref.shape[0]
    me = lax.axis_index("dp").astype(jnp.int32)
    head = x_ref[...].astype(jnp.float32)
    row = lax.broadcasted_iota(jnp.int32, (n, slots, part), 1)
    tail = jnp.zeros((n, slots, part), jnp.float32)
    for q in range(PARTS - 1):
        piece = head[:, :, q * part : (q + 1) * part]
        tail = jnp.where(row == q, piece[:, MOST : MOST + 1], tail)
        tail = jnp.where(row == q + THIRDS, piece[:, MOST + 1 : MOST + 2], tail)
    x = jnp.concatenate([head.reshape(rows, packed), tail.reshape(rows, part)], axis=1)
    x = x.astype(jnp.bfloat16)
    logits = lax.dot_general(
        x, router_ref[...], (((1,), (1,)), ((), ())), preferred_element_type=jnp.float32
    )
    expert_of = lax.broadcasted_iota(jnp.int32, logits.shape, 1)
    top = jnp.max(logits, axis=1, keepdims=True)
    weight = jnp.exp(logits - top)
    total = jnp.sum(weight, axis=1, keepdims=True)
    own = jnp.sum(jnp.where(expert_of == me, weight, 0.0), axis=1, keepdims=True)
    gate_value = (experts * (own / total)).astype(jnp.bfloat16).astype(jnp.float32)
    gate_act = jnp.dot(x, gate_ref[...], preferred_element_type=jnp.float32)
    up_act = jnp.dot(x, up_ref[...], preferred_element_type=jnp.float32)
    silu = gate_act / (1.0 + jnp.exp(-gate_act))
    hidden = (gate_value * silu * up_act).astype(jnp.bfloat16)
    y = jnp.dot(hidden, down_ref[...], preferred_element_type=jnp.float32)
    y = y.reshape(n, slots, width)
    last = y[:, :, packed:]
    for q in range(PARTS - 1):
        piece = y[:, :, q * part : (q + 1) * part]
        piece = jnp.where(row == MOST, last[:, q : q + 1], piece)
        piece = jnp.where(row == MOST + 1, last[:, q + THIRDS : q + THIRDS + 1], piece)
        y_ref[:, :, q * part : (q + 1) * part] = piece.astype(jnp.bfloat16)


def ffn(router_t, w_gate, w_up, w_down, x):
    return pl.pallas_call(
        ffn_kernel,
        out_shape=jax.ShapeDtypeStruct(x.shape, jnp.bfloat16),
        in_specs=[VMEM] * 5,
        out_specs=VMEM,
        compiler_params=PARAMS,
        name="ffn",
    )(router_t, w_gate, w_up, w_down, x)


def place(hot, rows):
    return lax.dot_general(hot, rows, (((0,), (0,)), ((), ())), preferred_element_type=jnp.float32)


def combine_kernel(hot_ref, y_ref, out_ref, block_ref, sem):
    n, slots, packed = y_ref.shape
    part = packed // (PARTS - 1)
    rows = n * slots
    copies = []
    pieces = [y_ref[:, :, q * part : (q + 1) * part] for q in range(PARTS - 1)]
    pieces = [p.astype(jnp.float32).reshape(rows, part).astype(jnp.bfloat16) for p in pieces]
    head = hot_ref[:rows]
    for q in range(PARTS):
        if q < PARTS - 1:
            total = place(head, pieces[q])
        else:
            total = place(hot_ref[rows:], jnp.concatenate(pieces, axis=0))
        block_ref[q] = total.astype(jnp.bfloat16)
        copy = pltpu.make_async_copy(
            block_ref.at[q], out_ref.at[:, pl.ds(q * part, part)], sem.at[q]
        )
        copy.start()
        copies.append(copy)
    for copy in copies:
        copy.wait()


def combine(hots, y):
    tok_dev = hots.shape[1]
    part = y.shape[2] // (PARTS - 1)
    return pl.pallas_call(
        combine_kernel,
        out_shape=jax.ShapeDtypeStruct((tok_dev, part * PARTS), jnp.bfloat16),
        in_specs=[VMEM, VMEM],
        out_specs=pl.BlockSpec(memory_space=pl.ANY),
        scratch_shapes=[
            pltpu.VMEM((PARTS, tok_dev, part), jnp.bfloat16),
            pltpu.SemaphoreType.DMA((PARTS,)),
        ],
        compiler_params=PARAMS,
        name="combine",
    )(hots, y)


def exchange(value):
    n = lax.axis_size("dp")
    order = [(n // 2 + 1 - k) % n for k in range(n)]
    return lax.all_to_all(
        value, "dp", split_axis=0, concat_axis=0, tiled=True, axis_index_groups=[order]
    )


def body(tokens, router, w_gate, w_up, w_down, picks):
    n = lax.axis_size("dp")
    send, hots = select(exchange(hold(jnp.broadcast_to(picks[None], (n,) + picks.shape))), tokens)
    received = exchange(send)
    y = ffn(router.T, w_gate[0], w_up[0], w_down[0], received)
    return combine(hots, exchange(y))


def solution(mesh):
    return jax.shard_map(
        body,
        mesh=mesh,
        in_specs=(
            P(("rep", "dp"), None),
            P("rep", None),
            P("dp", None, None),
            P("dp", None, None),
            P("dp", None, None),
            P(("rep", "dp"), None),
        ),
        out_specs=P(("rep", "dp"), None),
        check_vma=False,
    )
```

```python
import jax
import jax.numpy as jnp
from jax import lax
from jax.experimental import pallas as pl
from jax.experimental.pallas import tpu as pltpu
from jax.sharding import PartitionSpec as P

MOST = 6
SLOTS = 8
PARTS = 4
THIRDS = MOST // 2
LONG = 10_000_000_000
TALL = 128
VMEM = pl.BlockSpec(memory_space=pltpu.VMEM)
PARAMS = pltpu.CompilerParams(vmem_limit_bytes=16 * 1024 * 1024)


def hold_kernel(in_ref, out_ref):
    out_ref[...] = in_ref[...]


def hold(value):
    return pl.pallas_call(
        hold_kernel,
        out_shape=jax.ShapeDtypeStruct(value.shape, value.dtype),
        in_specs=[VMEM],
        out_specs=VMEM,
        compiler_params=PARAMS,
        cost_estimate=pl.CostEstimate(flops=LONG, bytes_accessed=0, transcendentals=0),
        name="hold",
    )(value)


def select_kernel(table_ref, tokens_ref, send_ref, hot_ref):
    tok_dev, width = tokens_ref.shape
    n, slots, _ = send_ref.shape
    capacity = table_ref.shape[2]
    part = width // PARTS
    me = lax.axis_index("dp").astype(jnp.int32)
    table = jnp.broadcast_to(table_ref[...], (n, slots, capacity))
    local = table - me * tok_dev
    row = lax.broadcasted_iota(jnp.int32, local.shape, 1)
    lane = lax.broadcasted_iota(jnp.int32, local.shape, 2)
    column = lax.broadcasted_iota(jnp.int32, (n, slots, tok_dev), 2)
    start = jnp.sum((local < 0).astype(jnp.int32), axis=2, keepdims=True)
    place = lane - start
    value = jnp.where((local >= 0) & (local < tok_dev), local + 1, 0)
    hots = []
    for q in range(PARTS):
        if q == 0:
            wanted = jnp.where(row < MOST, row, -1)
        else:
            first, second = q - 1, q - 1 + THIRDS
            wanted = jnp.where(row == MOST, first, jnp.where(row == MOST + 1, second, -1))
        index = jnp.sum(jnp.where(place == wanted, value, 0), axis=2, keepdims=True) - 1
        hot = (index == column).astype(jnp.float32).reshape(n * slots, tok_dev)
        hots.append(hot.astype(jnp.bfloat16))
        hot_ref[q * n * slots : (q + 1) * n * slots] = hots[q]
    rows = n * slots
    tails = jnp.dot(
        jnp.concatenate(hots[1:], axis=0),
        tokens_ref[:, (PARTS - 1) * part :],
        preferred_element_type=jnp.float32,
    )
    for q in range(PARTS - 1):
        chosen = jnp.dot(
            hots[0], tokens_ref[:, q * part : (q + 1) * part], preferred_element_type=jnp.float32
        )
        chosen = chosen + tails[q * rows : (q + 1) * rows]
        send_ref[:, :, q * part : (q + 1) * part] = chosen.reshape(n, slots, part).astype(
            jnp.bfloat16
        )


def select(table, tokens):
    tok_dev, width = tokens.shape
    n = table.shape[0]
    return pl.pallas_call(
        select_kernel,
        out_shape=[
            jax.ShapeDtypeStruct((n, SLOTS, width // PARTS * (PARTS - 1)), jnp.bfloat16),
            jax.ShapeDtypeStruct((PARTS * n * SLOTS, tok_dev), jnp.bfloat16),
        ],
        in_specs=[VMEM, VMEM],
        out_specs=[VMEM, VMEM],
        compiler_params=PARAMS,
        name="select",
    )(table, tokens)


def ffn_kernel(router_ref, gate_ref, up_ref, down_ref, x_ref, y_ref):
    n, slots, packed = x_ref.shape
    part = packed // (PARTS - 1)
    width = part * PARTS
    rows = n * slots
    experts = router_ref.shape[0]
    me = lax.axis_index("dp").astype(jnp.int32)
    head = x_ref[...].astype(jnp.float32)
    row = lax.broadcasted_iota(jnp.int32, (n, slots, part), 1)
    tail = jnp.zeros((n, slots, part), jnp.float32)
    for q in range(PARTS - 1):
        piece = head[:, :, q * part : (q + 1) * part]
        tail = jnp.where(row == q, piece[:, MOST : MOST + 1], tail)
        tail = jnp.where(row == q + THIRDS, piece[:, MOST + 1 : MOST + 2], tail)
    x = jnp.concatenate([head.reshape(rows, packed), tail.reshape(rows, part)], axis=1)
    x = x.astype(jnp.bfloat16)
    logits = lax.dot_general(
        x, router_ref[...], (((1,), (1,)), ((), ())), preferred_element_type=jnp.float32
    )
    expert_of = lax.broadcasted_iota(jnp.int32, logits.shape, 1)
    top = jnp.max(logits, axis=1, keepdims=True)
    weight = jnp.exp(logits - top)
    total = jnp.sum(weight, axis=1, keepdims=True)
    own = jnp.sum(jnp.where(expert_of == me, weight, 0.0), axis=1, keepdims=True)
    gate_value = (experts * (own / total)).astype(jnp.bfloat16).astype(jnp.float32)

    def product(left, right):
        if 2 * rows > TALL:
            return jnp.dot(left, right, preferred_element_type=jnp.float32)
        tall = jnp.concatenate([left, jnp.zeros_like(left)], axis=0)
        both = jnp.dot(tall, right, preferred_element_type=jnp.float32)
        return both[:rows] + both[rows:]

    gate_act = product(x, gate_ref[...])
    up_act = product(x, up_ref[...])
    silu = gate_act / (1.0 + jnp.exp(-gate_act))
    hidden = (gate_value * silu * up_act).astype(jnp.bfloat16)
    y = product(hidden, down_ref[...])
    y = y.reshape(n, slots, width)
    last = y[:, :, packed:]
    for q in range(PARTS - 1):
        piece = y[:, :, q * part : (q + 1) * part]
        piece = jnp.where(row == MOST, last[:, q : q + 1], piece)
        piece = jnp.where(row == MOST + 1, last[:, q + THIRDS : q + THIRDS + 1], piece)
        y_ref[:, :, q * part : (q + 1) * part] = piece.astype(jnp.bfloat16)


def ffn(router_t, w_gate, w_up, w_down, x):
    return pl.pallas_call(
        ffn_kernel,
        out_shape=jax.ShapeDtypeStruct(x.shape, jnp.bfloat16),
        in_specs=[VMEM] * 5,
        out_specs=VMEM,
        compiler_params=PARAMS,
        name="ffn",
    )(router_t, w_gate, w_up, w_down, x)


def place(hot, rows):
    return lax.dot_general(hot, rows, (((0,), (0,)), ((), ())), preferred_element_type=jnp.float32)


def combine_kernel(hot_ref, y_ref, out_ref, block_ref, sem):
    n, slots, packed = y_ref.shape
    part = packed // (PARTS - 1)
    rows = n * slots
    copies = []
    pieces = [y_ref[:, :, q * part : (q + 1) * part] for q in range(PARTS - 1)]
    pieces = [p.astype(jnp.float32).reshape(rows, part).astype(jnp.bfloat16) for p in pieces]
    head = hot_ref[:rows]
    for q in range(PARTS):
        if q < PARTS - 1:
            total = place(head, pieces[q])
        else:
            total = place(hot_ref[rows:], jnp.concatenate(pieces, axis=0))
        block_ref[q] = total.astype(jnp.bfloat16)
        copy = pltpu.make_async_copy(
            block_ref.at[q], out_ref.at[:, pl.ds(q * part, part)], sem.at[q]
        )
        copy.start()
        copies.append(copy)
    for copy in copies:
        copy.wait()


def combine(hots, y):
    tok_dev = hots.shape[1]
    part = y.shape[2] // (PARTS - 1)
    return pl.pallas_call(
        combine_kernel,
        out_shape=jax.ShapeDtypeStruct((tok_dev, part * PARTS), jnp.bfloat16),
        in_specs=[VMEM, VMEM],
        out_specs=pl.BlockSpec(memory_space=pl.ANY),
        scratch_shapes=[
            pltpu.VMEM((PARTS, tok_dev, part), jnp.bfloat16),
            pltpu.SemaphoreType.DMA((PARTS,)),
        ],
        compiler_params=PARAMS,
        name="combine",
    )(hots, y)


def ring(n):
    if n & (n - 1):
        return [(n // 2 + 1 - k) % n for k in range(n)]
    codes = [k ^ (k >> 1) for k in range(n)]
    return [(n // 2 + 1) % n ^ (c >> 1) ^ ((c & 1) * (n // 2)) for c in codes]


def exchange(value):
    return lax.all_to_all(
        value,
        "dp",
        split_axis=0,
        concat_axis=0,
        tiled=True,
        axis_index_groups=[ring(lax.axis_size("dp"))],
    )


def body(tokens, router, w_gate, w_up, w_down, picks):
    n = lax.axis_size("dp")
    send, hots = select(exchange(hold(jnp.broadcast_to(picks[None], (n,) + picks.shape))), tokens)
    received = exchange(send)
    y = ffn(router.T, w_gate[0], w_up[0], w_down[0], received)
    return combine(hots, exchange(y))


def solution(mesh):
    return jax.shard_map(
        body,
        mesh=mesh,
        in_specs=(
            P(("rep", "dp"), None),
            P("rep", None),
            P("dp", None, None),
            P("dp", None, None),
            P("dp", None, None),
            P(("rep", "dp"), None),
        ),
        out_specs=P(("rep", "dp"), None),
        check_vma=False,
    )
```

```python
import jax
import jax.numpy as jnp
from jax import lax
from jax.experimental import pallas as pl
from jax.experimental.pallas import tpu as pltpu
from jax.sharding import PartitionSpec as P

MOST = 6
SLOTS = 8
PARTS = 4
THIRDS = MOST // 2
LONG = 10_000_000_000
TALL = 128
VMEM = pl.BlockSpec(memory_space=pltpu.VMEM)
PARAMS = pltpu.CompilerParams(vmem_limit_bytes=16 * 1024 * 1024)


def hold_kernel(in_ref, out_ref):
    out_ref[...] = in_ref[...]


def hold(value):
    return pl.pallas_call(
        hold_kernel,
        out_shape=jax.ShapeDtypeStruct(value.shape, value.dtype),
        in_specs=[VMEM],
        out_specs=VMEM,
        compiler_params=PARAMS,
        cost_estimate=pl.CostEstimate(flops=LONG, bytes_accessed=0, transcendentals=0),
        name="hold",
    )(value)


def select_kernel(table_ref, tokens_ref, send_ref, hot_ref):
    tok_dev, width = tokens_ref.shape
    n, slots, _ = send_ref.shape
    capacity = table_ref.shape[2]
    part = width // PARTS
    me = lax.axis_index("dp").astype(jnp.int32)
    table = jnp.broadcast_to(table_ref[...], (n, slots, capacity))
    local = table - me * tok_dev
    row = lax.broadcasted_iota(jnp.int32, local.shape, 1)
    lane = lax.broadcasted_iota(jnp.int32, local.shape, 2)
    column = lax.broadcasted_iota(jnp.int32, (n, slots, tok_dev), 2)
    start = jnp.sum((local < 0).astype(jnp.int32), axis=2, keepdims=True)
    place = lane - start
    value = jnp.where((local >= 0) & (local < tok_dev), local + 1, 0)
    hots = []
    for q in range(PARTS):
        if q == 0:
            wanted = jnp.where(row < MOST, row, -1)
        else:
            first, second = q - 1, q - 1 + THIRDS
            wanted = jnp.where(row == MOST, first, jnp.where(row == MOST + 1, second, -1))
        index = jnp.sum(jnp.where(place == wanted, value, 0), axis=2, keepdims=True) - 1
        hot = (index == column).astype(jnp.float32).reshape(n * slots, tok_dev)
        hots.append(hot.astype(jnp.bfloat16))
        spot = (q + PARTS - 1) % PARTS * n * slots
        hot_ref[spot : spot + n * slots] = hots[q]
    rows = n * slots
    tails = jnp.dot(
        jnp.concatenate(hots[1:], axis=0),
        tokens_ref[:, (PARTS - 1) * part :],
        preferred_element_type=jnp.float32,
    )
    for q in range(PARTS - 1):
        chosen = jnp.dot(
            hots[0], tokens_ref[:, q * part : (q + 1) * part], preferred_element_type=jnp.float32
        )
        chosen = chosen + tails[q * rows : (q + 1) * rows]
        send_ref[:, :, q * part : (q + 1) * part] = chosen.reshape(n, slots, part).astype(
            jnp.bfloat16
        )


def select(table, tokens):
    tok_dev, width = tokens.shape
    n = table.shape[0]
    return pl.pallas_call(
        select_kernel,
        out_shape=[
            jax.ShapeDtypeStruct((n, SLOTS, width // PARTS * (PARTS - 1)), jnp.bfloat16),
            jax.ShapeDtypeStruct((PARTS * n * SLOTS, tok_dev), jnp.bfloat16),
        ],
        in_specs=[VMEM, VMEM],
        out_specs=[VMEM, VMEM],
        compiler_params=PARAMS,
        name="select",
    )(table, tokens)


def ffn_kernel(router_ref, gate_ref, up_ref, down_ref, hot_ref, x_ref, y_ref, turned_ref):
    n, slots, packed = x_ref.shape
    part = packed // (PARTS - 1)
    rows = n * slots
    experts = router_ref.shape[0]
    me = lax.axis_index("dp").astype(jnp.int32)
    head = x_ref[...].astype(jnp.float32)
    row = lax.broadcasted_iota(jnp.int32, (n, slots, part), 1)
    tail = jnp.zeros((n, slots, part), jnp.float32)
    for q in range(PARTS - 1):
        piece = head[:, :, q * part : (q + 1) * part]
        tail = jnp.where(row == q, piece[:, MOST : MOST + 1], tail)
        tail = jnp.where(row == q + THIRDS, piece[:, MOST + 1 : MOST + 2], tail)
    x = jnp.concatenate([head.reshape(rows, packed), tail.reshape(rows, part)], axis=1)
    x = x.astype(jnp.bfloat16)
    logits = lax.dot_general(
        x, router_ref[...], (((1,), (1,)), ((), ())), preferred_element_type=jnp.float32
    )
    expert_of = lax.broadcasted_iota(jnp.int32, logits.shape, 1)
    top = jnp.max(logits, axis=1, keepdims=True)
    weight = jnp.exp(logits - top)
    total = jnp.sum(weight, axis=1, keepdims=True)
    own = jnp.sum(jnp.where(expert_of == me, weight, 0.0), axis=1, keepdims=True)
    gate_value = (experts * (own / total)).astype(jnp.bfloat16).astype(jnp.float32)

    def product(left, right):
        if 2 * rows > TALL:
            return jnp.dot(left, right, preferred_element_type=jnp.float32)
        tall = jnp.concatenate([left, jnp.zeros_like(left)], axis=0)
        both = jnp.dot(tall, right, preferred_element_type=jnp.float32)
        return both[:rows] + both[rows:]

    gate_act = product(x, gate_ref[...])
    up_act = product(x, up_ref[...])
    silu = gate_act / (1.0 + jnp.exp(-gate_act))
    hidden = (gate_value * silu * up_act).astype(jnp.bfloat16)
    turned_ref[...] = hot_ref[...].T
    last = product(hidden, down_ref[:, packed:]).reshape(n, slots, part)
    for q in range(PARTS - 1):
        piece = product(hidden, down_ref[:, q * part : (q + 1) * part]).reshape(n, slots, part)
        piece = jnp.where(row == MOST, last[:, q : q + 1], piece)
        piece = jnp.where(row == MOST + 1, last[:, q + THIRDS : q + THIRDS + 1], piece)
        y_ref[:, :, q * part : (q + 1) * part] = piece.astype(jnp.bfloat16)


def ffn(router_t, w_gate, w_up, w_down, hots, x):
    return pl.pallas_call(
        ffn_kernel,
        out_shape=[
            jax.ShapeDtypeStruct(x.shape, jnp.bfloat16),
            jax.ShapeDtypeStruct(hots.shape[::-1], jnp.bfloat16),
        ],
        in_specs=[VMEM] * 6,
        out_specs=[VMEM, VMEM],
        compiler_params=PARAMS,
        name="ffn",
    )(router_t, w_gate, w_up, w_down, hots, x)


def combine_kernel(hot_ref, y_ref, out_ref, block_ref, sem):
    n, slots, packed = y_ref.shape
    part = packed // (PARTS - 1)
    rows = n * slots
    copies = []
    pieces = [y_ref[:, :, q * part : (q + 1) * part] for q in range(PARTS - 1)]
    pieces = [p.astype(jnp.float32).reshape(rows, part).astype(jnp.bfloat16) for p in pieces]
    blank = jnp.zeros_like(pieces[0])
    for q in range(PARTS):
        if q < PARTS - 1:
            hot, values = hot_ref[:, 2 * rows :], [blank, pieces[q]]
        else:
            hot, values = hot_ref[...], pieces + [blank]
        total = jnp.dot(
            hot, jnp.concatenate(values, axis=0), preferred_element_type=jnp.float32
        )
        block_ref[q] = total.astype(jnp.bfloat16)
        copy = pltpu.make_async_copy(
            block_ref.at[q], out_ref.at[:, pl.ds(q * part, part)], sem.at[q]
        )
        copy.start()
        copies.append(copy)
    for copy in copies:
        copy.wait()


def combine(hots, y):
    tok_dev = hots.shape[0]
    part = y.shape[2] // (PARTS - 1)
    return pl.pallas_call(
        combine_kernel,
        out_shape=jax.ShapeDtypeStruct((tok_dev, part * PARTS), jnp.bfloat16),
        in_specs=[VMEM, VMEM],
        out_specs=pl.BlockSpec(memory_space=pl.ANY),
        scratch_shapes=[
            pltpu.VMEM((PARTS, tok_dev, part), jnp.bfloat16),
            pltpu.SemaphoreType.DMA((PARTS,)),
        ],
        compiler_params=PARAMS,
        name="combine",
    )(hots, y)


def ring(n):
    if n & (n - 1):
        return [(n // 2 + 1 - k) % n for k in range(n)]
    codes = [k ^ (k >> 1) for k in range(n)]
    return [(n // 2 + 1) % n ^ (c >> 1) ^ ((c & 1) * (n // 2)) for c in codes]


def exchange(value):
    return lax.all_to_all(
        value,
        "dp",
        split_axis=0,
        concat_axis=0,
        tiled=True,
        axis_index_groups=[ring(lax.axis_size("dp"))],
    )


def body(tokens, router, w_gate, w_up, w_down, picks):
    n = lax.axis_size("dp")
    send, hots = select(exchange(hold(jnp.broadcast_to(picks[None], (n,) + picks.shape))), tokens)
    received = exchange(send)
    y, turned = ffn(router.T, w_gate[0], w_up[0], w_down[0], hots, received)
    return combine(turned, exchange(y))


def solution(mesh):
    return jax.shard_map(
        body,
        mesh=mesh,
        in_specs=(
            P(("rep", "dp"), None),
            P("rep", None),
            P("dp", None, None),
            P("dp", None, None),
            P("dp", None, None),
            P(("rep", "dp"), None),
        ),
        out_specs=P(("rep", "dp"), None),
        check_vma=False,
    )
```

```python
import jax
import jax.numpy as jnp
from jax import lax
from jax.experimental import pallas as pl
from jax.experimental.pallas import tpu as pltpu
from jax.sharding import PartitionSpec as P

MOST = 6
SLOTS = 8
PARTS = 4
THIRDS = MOST // 2
LONG = 10_000_000_000
TALL = 128
VMEM = pl.BlockSpec(memory_space=pltpu.VMEM)
PARAMS = pltpu.CompilerParams(vmem_limit_bytes=16 * 1024 * 1024)


def hold_kernel(in_ref, out_ref):
    out_ref[...] = in_ref[...]


def hold(value):
    return pl.pallas_call(
        hold_kernel,
        out_shape=jax.ShapeDtypeStruct(value.shape, value.dtype),
        in_specs=[VMEM],
        out_specs=VMEM,
        compiler_params=PARAMS,
        cost_estimate=pl.CostEstimate(flops=LONG, bytes_accessed=0, transcendentals=0),
        name="hold",
    )(value)


def select_kernel(table_ref, tokens_ref, send_ref, hot_ref):
    tok_dev, width = tokens_ref.shape
    n, _, capacity = table_ref.shape
    slots = SLOTS
    part = width // PARTS
    me = lax.axis_index("dp").astype(jnp.int32)
    table = jnp.broadcast_to(table_ref[...], (n, slots, capacity))
    local = table - me * tok_dev
    row = lax.broadcasted_iota(jnp.int32, local.shape, 1)
    lane = lax.broadcasted_iota(jnp.int32, local.shape, 2)
    column = lax.broadcasted_iota(jnp.int32, (n, slots, tok_dev), 2)
    start = jnp.sum((local < 0).astype(jnp.int32), axis=2, keepdims=True)
    place = lane - start
    value = jnp.where((local >= 0) & (local < tok_dev), local + 1, 0)
    hots = []
    for q in range(PARTS):
        if q == 0:
            wanted = jnp.where(row < MOST, row, -1)
        else:
            first, second = q - 1, q - 1 + THIRDS
            wanted = jnp.where(row == MOST, first, jnp.where(row == MOST + 1, second, -1))
        index = jnp.sum(jnp.where(place == wanted, value, 0), axis=2, keepdims=True) - 1
        hot = (index == column).astype(jnp.float32).reshape(n * slots, tok_dev)
        hots.append(hot.astype(jnp.bfloat16))
        spot = (q + PARTS - 1) % PARTS * n * slots
        hot_ref[spot : spot + n * slots] = hots[q]
    rows = n * slots
    tails = jnp.dot(
        jnp.concatenate(hots[1:], axis=0),
        tokens_ref[:, (PARTS - 1) * part :],
        preferred_element_type=jnp.float32,
    )
    for q in range(PARTS - 1):
        chosen = jnp.dot(
            hots[0], tokens_ref[:, q * part : (q + 1) * part], preferred_element_type=jnp.float32
        )
        chosen = chosen + tails[q * rows : (q + 1) * rows]
        send_ref[:, q * part : (q + 1) * part] = chosen.astype(jnp.bfloat16)


def select(table, tokens):
    tok_dev, width = tokens.shape
    n = table.shape[0]
    return pl.pallas_call(
        select_kernel,
        out_shape=[
            jax.ShapeDtypeStruct((n * SLOTS, width // PARTS * (PARTS - 1)), jnp.bfloat16),
            jax.ShapeDtypeStruct((PARTS * n * SLOTS, tok_dev), jnp.bfloat16),
        ],
        in_specs=[VMEM, VMEM],
        out_specs=[VMEM, VMEM],
        compiler_params=PARAMS,
        name="select",
    )(table, tokens)


def ffn_kernel(router_ref, gate_ref, up_ref, down_ref, hot_ref, x_ref, y_ref, turned_ref):
    rows, packed = x_ref.shape
    part = packed // (PARTS - 1)
    n, slots = rows // SLOTS, SLOTS
    experts = router_ref.shape[0]
    me = lax.axis_index("dp").astype(jnp.int32)
    row = lax.broadcasted_iota(jnp.int32, (n, slots, part), 1)
    tail = jnp.zeros((n, slots, part), jnp.float32)
    for q in range(PARTS - 1):
        piece = x_ref[:, q * part : (q + 1) * part].astype(jnp.float32).reshape(n, slots, part)
        tail = jnp.where(row == q, piece[:, MOST : MOST + 1], tail)
        tail = jnp.where(row == q + THIRDS, piece[:, MOST + 1 : MOST + 2], tail)
    x = jnp.concatenate([x_ref[...], tail.reshape(rows, part).astype(jnp.bfloat16)], axis=1)
    logits = lax.dot_general(
        x, router_ref[...], (((1,), (1,)), ((), ())), preferred_element_type=jnp.float32
    )
    expert_of = lax.broadcasted_iota(jnp.int32, logits.shape, 1)
    top = jnp.max(logits, axis=1, keepdims=True)
    weight = jnp.exp(logits - top)
    total = jnp.sum(weight, axis=1, keepdims=True)
    own = jnp.sum(jnp.where(expert_of == me, weight, 0.0), axis=1, keepdims=True)
    gate_value = (experts * (own / total)).astype(jnp.bfloat16).astype(jnp.float32)

    def product(left, right):
        if 2 * rows > TALL:
            return jnp.dot(left, right, preferred_element_type=jnp.float32)
        tall = jnp.concatenate([left, jnp.zeros_like(left)], axis=0)
        both = jnp.dot(tall, right, preferred_element_type=jnp.float32)
        return both[:rows] + both[rows:]

    gate_act = product(x, gate_ref[...])
    up_act = product(x, up_ref[...])
    silu = gate_act / (1.0 + jnp.exp(-gate_act))
    hidden = (gate_value * silu * up_act).astype(jnp.bfloat16)
    turned_ref[...] = hot_ref[...].T
    last = product(hidden, down_ref[:, packed:]).reshape(n, slots, part)
    for q in range(PARTS - 1):
        piece = product(hidden, down_ref[:, q * part : (q + 1) * part]).reshape(n, slots, part)
        piece = jnp.where(row == MOST, last[:, q : q + 1], piece)
        piece = jnp.where(row == MOST + 1, last[:, q + THIRDS : q + THIRDS + 1], piece)
        y_ref[:, q * part : (q + 1) * part] = piece.reshape(rows, part).astype(jnp.bfloat16)


def ffn(router_t, w_gate, w_up, w_down, hots, x):
    return pl.pallas_call(
        ffn_kernel,
        out_shape=[
            jax.ShapeDtypeStruct(x.shape, jnp.bfloat16),
            jax.ShapeDtypeStruct(hots.shape[::-1], jnp.bfloat16),
        ],
        in_specs=[VMEM] * 6,
        out_specs=[VMEM, VMEM],
        compiler_params=PARAMS,
        name="ffn",
    )(router_t, w_gate, w_up, w_down, hots, x)


def combine_kernel(hot_ref, y_ref, out_ref, block_ref, sem):
    rows, packed = y_ref.shape
    part = packed // (PARTS - 1)
    copies = []
    pieces = [y_ref[:, q * part : (q + 1) * part] for q in range(PARTS - 1)]
    blank = jnp.zeros_like(pieces[0])
    for q in range(PARTS):
        if q < PARTS - 1:
            hot, values = hot_ref[:, 2 * rows :], [blank, pieces[q]]
        else:
            hot, values = hot_ref[...], pieces + [blank]
        total = jnp.dot(
            hot, jnp.concatenate(values, axis=0), preferred_element_type=jnp.float32
        )
        block_ref[q] = total.astype(jnp.bfloat16)
        copy = pltpu.make_async_copy(
            block_ref.at[q], out_ref.at[:, pl.ds(q * part, part)], sem.at[q]
        )
        copy.start()
        copies.append(copy)
    for copy in copies:
        copy.wait()


def combine(hots, y):
    tok_dev = hots.shape[0]
    part = y.shape[1] // (PARTS - 1)
    return pl.pallas_call(
        combine_kernel,
        out_shape=jax.ShapeDtypeStruct((tok_dev, part * PARTS), jnp.bfloat16),
        in_specs=[VMEM, VMEM],
        out_specs=pl.BlockSpec(memory_space=pl.ANY),
        scratch_shapes=[
            pltpu.VMEM((PARTS, tok_dev, part), jnp.bfloat16),
            pltpu.SemaphoreType.DMA((PARTS,)),
        ],
        compiler_params=PARAMS,
        name="combine",
    )(hots, y)


def ring(n):
    if n & (n - 1):
        return [(n // 2 + 1 - k) % n for k in range(n)]
    codes = [k ^ (k >> 1) for k in range(n)]
    return [(n // 2 + 1) % n ^ (c >> 1) ^ ((c & 1) * (n // 2)) for c in codes]


def exchange(value):
    return lax.all_to_all(
        value,
        "dp",
        split_axis=0,
        concat_axis=0,
        tiled=True,
        axis_index_groups=[ring(lax.axis_size("dp"))],
    )


def swap(rows, n):
    return exchange(rows.reshape(n, SLOTS, rows.shape[1])).reshape(rows.shape)


def body(tokens, router, w_gate, w_up, w_down, picks):
    n = lax.axis_size("dp")
    table = exchange(hold(jnp.broadcast_to(picks[None], (n,) + picks.shape)))
    send, hots = select(table, tokens)
    received = swap(send, n)
    y, turned = ffn(router.T, w_gate[0], w_up[0], w_down[0], hots, received)
    return combine(turned, swap(y, n))


def solution(mesh):
    return jax.shard_map(
        body,
        mesh=mesh,
        in_specs=(
            P(("rep", "dp"), None),
            P("rep", None),
            P("dp", None, None),
            P("dp", None, None),
            P("dp", None, None),
            P(("rep", "dp"), None),
        ),
        out_specs=P(("rep", "dp"), None),
        check_vma=False,
    )
```

```python
import jax
import jax.numpy as jnp
from jax import lax
from jax.experimental import pallas as pl
from jax.experimental.pallas import tpu as pltpu
from jax.sharding import PartitionSpec as P

MOST = 6
SLOTS = 8
PARTS = 4
THIRDS = MOST // 2
LONG = 10_000_000_000
TALL = 128
VMEM = pl.BlockSpec(memory_space=pltpu.VMEM)
PARAMS = pltpu.CompilerParams(vmem_limit_bytes=16 * 1024 * 1024)


def hold_kernel(picks_ref, out_ref, row_ref, sem):
    copy = pltpu.make_async_copy(picks_ref, row_ref, sem)
    copy.start()
    copy.wait()
    out_ref[...] = jnp.broadcast_to(row_ref[...][None], out_ref.shape)


def hold(picks, n):
    return pl.pallas_call(
        hold_kernel,
        out_shape=jax.ShapeDtypeStruct((n,) + picks.shape, picks.dtype),
        in_specs=[pl.BlockSpec(memory_space=pltpu.HBM)],
        out_specs=VMEM,
        scratch_shapes=[pltpu.VMEM(picks.shape, picks.dtype), pltpu.SemaphoreType.DMA],
        compiler_params=PARAMS,
        cost_estimate=pl.CostEstimate(flops=LONG, bytes_accessed=0, transcendentals=0),
        name="hold",
    )(picks)


def select_kernel(table_ref, tokens_ref, send_ref, hot_ref):
    tok_dev, width = tokens_ref.shape
    n, _, capacity = table_ref.shape
    slots = SLOTS
    part = width // PARTS
    me = lax.axis_index("dp").astype(jnp.int32)
    table = jnp.broadcast_to(table_ref[...], (n, slots, capacity))
    local = table - me * tok_dev
    row = lax.broadcasted_iota(jnp.int32, local.shape, 1)
    lane = lax.broadcasted_iota(jnp.int32, local.shape, 2)
    column = lax.broadcasted_iota(jnp.int32, (n, slots, tok_dev), 2)
    start = jnp.sum((local < 0).astype(jnp.int32), axis=2, keepdims=True)
    place = lane - start
    value = jnp.where((local >= 0) & (local < tok_dev), local + 1, 0)
    hots = []
    for q in range(PARTS):
        if q == 0:
            wanted = jnp.where(row < MOST, row, -1)
        else:
            first, second = q - 1, q - 1 + THIRDS
            wanted = jnp.where(row == MOST, first, jnp.where(row == MOST + 1, second, -1))
        index = jnp.sum(jnp.where(place == wanted, value, 0), axis=2, keepdims=True) - 1
        hot = (index == column).astype(jnp.float32).reshape(n * slots, tok_dev)
        hots.append(hot.astype(jnp.bfloat16))
        spot = (q + PARTS - 1) % PARTS * n * slots
        hot_ref[spot : spot + n * slots] = hots[q]
    rows = n * slots
    tails = jnp.dot(
        jnp.concatenate(hots[1:], axis=0),
        tokens_ref[:, (PARTS - 1) * part :],
        preferred_element_type=jnp.float32,
    )
    for q in range(PARTS - 1):
        chosen = jnp.dot(
            hots[0], tokens_ref[:, q * part : (q + 1) * part], preferred_element_type=jnp.float32
        )
        chosen = chosen + tails[q * rows : (q + 1) * rows]
        send_ref[:, q * part : (q + 1) * part] = chosen.astype(jnp.bfloat16)


def select(table, tokens):
    tok_dev, width = tokens.shape
    n = table.shape[0]
    return pl.pallas_call(
        select_kernel,
        out_shape=[
            jax.ShapeDtypeStruct((n * SLOTS, width // PARTS * (PARTS - 1)), jnp.bfloat16),
            jax.ShapeDtypeStruct((PARTS * n * SLOTS, tok_dev), jnp.bfloat16),
        ],
        in_specs=[VMEM, VMEM],
        out_specs=[VMEM, VMEM],
        compiler_params=PARAMS,
        name="select",
    )(table, tokens)


def ffn_kernel(router_ref, gate_ref, up_ref, down_ref, hot_ref, x_ref, y_ref, turned_ref):
    rows, packed = x_ref.shape
    part = packed // (PARTS - 1)
    n, slots = rows // SLOTS, SLOTS
    experts = router_ref.shape[0]
    me = lax.axis_index("dp").astype(jnp.int32)
    row = lax.broadcasted_iota(jnp.int32, (n, slots, part), 1)
    tail = jnp.zeros((n, slots, part), jnp.float32)
    for q in range(PARTS - 1):
        piece = x_ref[:, q * part : (q + 1) * part].astype(jnp.float32).reshape(n, slots, part)
        tail = jnp.where(row == q, piece[:, MOST : MOST + 1], tail)
        tail = jnp.where(row == q + THIRDS, piece[:, MOST + 1 : MOST + 2], tail)
    x = jnp.concatenate([x_ref[...], tail.reshape(rows, part).astype(jnp.bfloat16)], axis=1)
    logits = lax.dot_general(
        x, router_ref[...], (((1,), (1,)), ((), ())), preferred_element_type=jnp.float32
    )
    expert_of = lax.broadcasted_iota(jnp.int32, logits.shape, 1)
    top = jnp.max(logits, axis=1, keepdims=True)
    weight = jnp.exp(logits - top)
    total = jnp.sum(weight, axis=1, keepdims=True)
    own = jnp.sum(jnp.where(expert_of == me, weight, 0.0), axis=1, keepdims=True)
    gate_value = (experts * (own / total)).astype(jnp.bfloat16).astype(jnp.float32)

    def product(left, right):
        if 2 * rows > TALL:
            return jnp.dot(left, right, preferred_element_type=jnp.float32)
        tall = jnp.concatenate([left, jnp.zeros_like(left)], axis=0)
        both = jnp.dot(tall, right, preferred_element_type=jnp.float32)
        return both[:rows] + both[rows:]

    gate_act = product(x, gate_ref[...])
    up_act = product(x, up_ref[...])
    silu = gate_act / (1.0 + jnp.exp(-gate_act))
    hidden = (gate_value * silu * up_act).astype(jnp.bfloat16)
    turned_ref[...] = hot_ref[...].T
    last = product(hidden, down_ref[:, packed:]).reshape(n, slots, part)
    for q in range(PARTS - 1):
        piece = product(hidden, down_ref[:, q * part : (q + 1) * part]).reshape(n, slots, part)
        piece = jnp.where(row == MOST, last[:, q : q + 1], piece)
        piece = jnp.where(row == MOST + 1, last[:, q + THIRDS : q + THIRDS + 1], piece)
        y_ref[:, q * part : (q + 1) * part] = piece.reshape(rows, part).astype(jnp.bfloat16)


def ffn(router_t, w_gate, w_up, w_down, hots, x):
    return pl.pallas_call(
        ffn_kernel,
        out_shape=[
            jax.ShapeDtypeStruct(x.shape, jnp.bfloat16),
            jax.ShapeDtypeStruct(hots.shape[::-1], jnp.bfloat16),
        ],
        in_specs=[VMEM] * 6,
        out_specs=[VMEM, VMEM],
        compiler_params=PARAMS,
        name="ffn",
    )(router_t, w_gate, w_up, w_down, hots, x)


def combine_kernel(hot_ref, y_ref, out_ref, block_ref, sem):
    rows, packed = y_ref.shape
    part = packed // (PARTS - 1)
    copies = []
    pieces = [y_ref[:, q * part : (q + 1) * part] for q in range(PARTS - 1)]
    blank = jnp.zeros_like(pieces[0])
    for q in range(PARTS):
        if q < PARTS - 1:
            hot, values = hot_ref[:, 2 * rows :], [blank, pieces[q]]
        else:
            hot, values = hot_ref[...], pieces + [blank]
        total = jnp.dot(
            hot, jnp.concatenate(values, axis=0), preferred_element_type=jnp.float32
        )
        block_ref[q] = total.astype(jnp.bfloat16)
        copy = pltpu.make_async_copy(
            block_ref.at[q], out_ref.at[:, pl.ds(q * part, part)], sem.at[q]
        )
        copy.start()
        copies.append(copy)
    for copy in copies:
        copy.wait()


def combine(hots, y):
    tok_dev = hots.shape[0]
    part = y.shape[1] // (PARTS - 1)
    return pl.pallas_call(
        combine_kernel,
        out_shape=jax.ShapeDtypeStruct((tok_dev, part * PARTS), jnp.bfloat16),
        in_specs=[VMEM, VMEM],
        out_specs=pl.BlockSpec(memory_space=pl.ANY),
        scratch_shapes=[
            pltpu.VMEM((PARTS, tok_dev, part), jnp.bfloat16),
            pltpu.SemaphoreType.DMA((PARTS,)),
        ],
        compiler_params=PARAMS,
        name="combine",
    )(hots, y)


def ring(n):
    if n & (n - 1):
        return [(n // 2 + 1 - k) % n for k in range(n)]
    codes = [k ^ (k >> 1) for k in range(n)]
    return [(n // 2 + 1) % n ^ (c >> 1) ^ ((c & 1) * (n // 2)) for c in codes]


def exchange(value):
    return lax.all_to_all(
        value,
        "dp",
        split_axis=0,
        concat_axis=0,
        tiled=True,
        axis_index_groups=[ring(lax.axis_size("dp"))],
    )


def swap(rows, n):
    return exchange(rows.reshape(n, SLOTS, rows.shape[1])).reshape(rows.shape)


def body(tokens, router, w_gate, w_up, w_down, picks):
    n = lax.axis_size("dp")
    table = exchange(hold(picks, n))
    send, hots = select(table, tokens)
    received = swap(send, n)
    y, turned = ffn(router.T, w_gate[0], w_up[0], w_down[0], hots, received)
    return combine(turned, swap(y, n))


def solution(mesh):
    return jax.shard_map(
        body,
        mesh=mesh,
        in_specs=(
            P(("rep", "dp"), None),
            P("rep", None),
            P("dp", None, None),
            P("dp", None, None),
            P("dp", None, None),
            P(("rep", "dp"), None),
        ),
        out_specs=P(("rep", "dp"), None),
        check_vma=False,
    )
```

```python
import jax
import jax.numpy as jnp
from jax import lax
from jax.experimental import pallas as pl
from jax.experimental.pallas import tpu as pltpu
from jax.sharding import PartitionSpec as P

MOST = 6
SLOTS = 8
PARTS = 4
THIRDS = MOST // 2
LONG = 10_000_000_000
TALL = 128
VMEM = pl.BlockSpec(memory_space=pltpu.VMEM)
PARAMS = pltpu.CompilerParams(vmem_limit_bytes=16 * 1024 * 1024)


def hold_kernel(in_ref, out_ref):
    out_ref[...] = in_ref[...]


def hold(value):
    return pl.pallas_call(
        hold_kernel,
        out_shape=jax.ShapeDtypeStruct(value.shape, value.dtype),
        in_specs=[VMEM],
        out_specs=VMEM,
        compiler_params=PARAMS,
        cost_estimate=pl.CostEstimate(flops=LONG, bytes_accessed=0, transcendentals=0),
        name="hold",
    )(value)


def select_kernel(table_ref, tokens_ref, send_ref, hot_ref):
    tok_dev, width = tokens_ref.shape
    n, _, capacity = table_ref.shape
    slots = SLOTS
    part = width // PARTS
    me = lax.axis_index("dp").astype(jnp.int32)
    table = jnp.broadcast_to(table_ref[...], (n, slots, capacity))
    local = table - me * tok_dev
    row = lax.broadcasted_iota(jnp.int32, local.shape, 1)
    lane = lax.broadcasted_iota(jnp.int32, local.shape, 2)
    column = lax.broadcasted_iota(jnp.int32, (n * slots, tok_dev), 1).astype(jnp.int16)
    one, zero = jnp.bfloat16(1), jnp.bfloat16(0)
    start = jnp.sum((local < 0).astype(jnp.int32), axis=2, keepdims=True)
    place = lane - start
    value = jnp.where((local >= 0) & (local < tok_dev), local + 1, 0)
    hots = []
    for q in range(PARTS):
        if q == 0:
            wanted = jnp.where(row < MOST, row, -1)
        else:
            first, second = q - 1, q - 1 + THIRDS
            wanted = jnp.where(row == MOST, first, jnp.where(row == MOST + 1, second, -1))
        index = jnp.sum(jnp.where(place == wanted, value, 0), axis=2, keepdims=True) - 1
        spread = jnp.broadcast_to(index, (n, slots, 128)).reshape(n * slots, 128).astype(jnp.int16)
        hot = [
            jnp.where(spread == column[:, c : c + 128], one, zero)
            for c in range(0, tok_dev, 128)
        ]
        hots.append(jnp.concatenate(hot, axis=1))
        spot = (q + PARTS - 1) % PARTS * n * slots
        hot_ref[spot : spot + n * slots] = hots[q]
    rows = n * slots
    tails = jnp.dot(
        jnp.concatenate(hots[1:], axis=0),
        tokens_ref[:, (PARTS - 1) * part :],
        preferred_element_type=jnp.float32,
    )
    for q in range(PARTS - 1):
        chosen = jnp.dot(
            hots[0], tokens_ref[:, q * part : (q + 1) * part], preferred_element_type=jnp.float32
        )
        chosen = chosen + tails[q * rows : (q + 1) * rows]
        send_ref[:, q * part : (q + 1) * part] = chosen.astype(jnp.bfloat16)


def select(table, tokens):
    tok_dev, width = tokens.shape
    n = table.shape[0]
    return pl.pallas_call(
        select_kernel,
        out_shape=[
            jax.ShapeDtypeStruct((n * SLOTS, width // PARTS * (PARTS - 1)), jnp.bfloat16),
            jax.ShapeDtypeStruct((PARTS * n * SLOTS, tok_dev), jnp.bfloat16),
        ],
        in_specs=[VMEM, VMEM],
        out_specs=[VMEM, VMEM],
        compiler_params=PARAMS,
        name="select",
    )(table, tokens)


def ffn_kernel(router_ref, gate_ref, up_ref, down_ref, hot_ref, x_ref, y_ref, turned_ref):
    rows, packed = x_ref.shape
    part = packed // (PARTS - 1)
    n, slots = rows // SLOTS, SLOTS
    experts = router_ref.shape[0]
    me = lax.axis_index("dp").astype(jnp.int32)
    row = lax.broadcasted_iota(jnp.int32, (n, slots, part), 1)
    tail = jnp.zeros((n, slots, part), jnp.float32)
    for q in range(PARTS - 1):
        piece = x_ref[:, q * part : (q + 1) * part].astype(jnp.float32).reshape(n, slots, part)
        tail = jnp.where(row == q, piece[:, MOST : MOST + 1], tail)
        tail = jnp.where(row == q + THIRDS, piece[:, MOST + 1 : MOST + 2], tail)
    x = jnp.concatenate([x_ref[...], tail.reshape(rows, part).astype(jnp.bfloat16)], axis=1)
    logits = lax.dot_general(
        x, router_ref[...], (((1,), (1,)), ((), ())), preferred_element_type=jnp.float32
    )
    expert_of = lax.broadcasted_iota(jnp.int32, logits.shape, 1)
    top = jnp.max(logits, axis=1, keepdims=True)
    weight = jnp.exp(logits - top)
    total = jnp.sum(weight, axis=1, keepdims=True)
    own = jnp.sum(jnp.where(expert_of == me, weight, 0.0), axis=1, keepdims=True)
    gate_value = (experts * (own / total)).astype(jnp.bfloat16).astype(jnp.float32)

    def product(left, right):
        if 2 * rows > TALL:
            return jnp.dot(left, right, preferred_element_type=jnp.float32)
        tall = jnp.concatenate([left, jnp.zeros_like(left)], axis=0)
        both = jnp.dot(tall, right, preferred_element_type=jnp.float32)
        return both[:rows] + both[rows:]

    gate_act = product(x, gate_ref[...])
    up_act = product(x, up_ref[...])
    silu = gate_act / (1.0 + jnp.exp(-gate_act))
    hidden = (gate_value * silu * up_act).astype(jnp.bfloat16)
    turned_ref[...] = hot_ref[...].T
    last = product(hidden, down_ref[:, packed:]).reshape(n, slots, part)
    for q in range(PARTS - 1):
        piece = product(hidden, down_ref[:, q * part : (q + 1) * part]).reshape(n, slots, part)
        piece = jnp.where(row == MOST, last[:, q : q + 1], piece)
        piece = jnp.where(row == MOST + 1, last[:, q + THIRDS : q + THIRDS + 1], piece)
        y_ref[:, q * part : (q + 1) * part] = piece.reshape(rows, part).astype(jnp.bfloat16)


def ffn(router_t, w_gate, w_up, w_down, hots, x):
    return pl.pallas_call(
        ffn_kernel,
        out_shape=[
            jax.ShapeDtypeStruct(x.shape, jnp.bfloat16),
            jax.ShapeDtypeStruct(hots.shape[::-1], jnp.bfloat16),
        ],
        in_specs=[VMEM] * 6,
        out_specs=[VMEM, VMEM],
        compiler_params=PARAMS,
        name="ffn",
    )(router_t, w_gate, w_up, w_down, hots, x)


def combine_kernel(hot_ref, y_ref, out_ref, block_ref, sem):
    rows, packed = y_ref.shape
    part = packed // (PARTS - 1)
    copies = []
    pieces = [y_ref[:, q * part : (q + 1) * part] for q in range(PARTS - 1)]
    blank = jnp.zeros_like(pieces[0])
    for q in range(PARTS):
        if q < PARTS - 1:
            hot, values = hot_ref[:, 2 * rows :], [blank, pieces[q]]
        else:
            hot, values = hot_ref[...], pieces + [blank]
        total = jnp.dot(
            hot, jnp.concatenate(values, axis=0), preferred_element_type=jnp.float32
        )
        block_ref[q] = total.astype(jnp.bfloat16)
        copy = pltpu.make_async_copy(
            block_ref.at[q], out_ref.at[:, pl.ds(q * part, part)], sem.at[q]
        )
        copy.start()
        copies.append(copy)
    for copy in copies:
        copy.wait()


def combine(hots, y):
    tok_dev = hots.shape[0]
    part = y.shape[1] // (PARTS - 1)
    return pl.pallas_call(
        combine_kernel,
        out_shape=jax.ShapeDtypeStruct((tok_dev, part * PARTS), jnp.bfloat16),
        in_specs=[VMEM, VMEM],
        out_specs=pl.BlockSpec(memory_space=pl.ANY),
        scratch_shapes=[
            pltpu.VMEM((PARTS, tok_dev, part), jnp.bfloat16),
            pltpu.SemaphoreType.DMA((PARTS,)),
        ],
        compiler_params=PARAMS,
        name="combine",
    )(hots, y)


def ring(n):
    if n & (n - 1):
        return [(n // 2 + 1 - k) % n for k in range(n)]
    codes = [k ^ (k >> 1) for k in range(n)]
    return [(n // 2 + 1) % n ^ (c >> 1) ^ ((c & 1) * (n // 2)) for c in codes]


def exchange(value):
    return lax.all_to_all(
        value,
        "dp",
        split_axis=0,
        concat_axis=0,
        tiled=True,
        axis_index_groups=[ring(lax.axis_size("dp"))],
    )


def swap(rows, n):
    return exchange(rows.reshape(n, SLOTS, rows.shape[1])).reshape(rows.shape)


def body(tokens, router, w_gate, w_up, w_down, picks):
    n = lax.axis_size("dp")
    table = exchange(hold(jnp.broadcast_to(picks[None], (n,) + picks.shape)))
    send, hots = select(table, tokens)
    received = swap(send, n)
    y, turned = ffn(router.T, w_gate[0], w_up[0], w_down[0], hots, received)
    return combine(turned, swap(y, n))


def solution(mesh):
    return jax.shard_map(
        body,
        mesh=mesh,
        in_specs=(
            P(("rep", "dp"), None),
            P("rep", None),
            P("dp", None, None),
            P("dp", None, None),
            P("dp", None, None),
            P(("rep", "dp"), None),
        ),
        out_specs=P(("rep", "dp"), None),
        check_vma=False,
    )
```
